32 devices in a mesh: dom: 4 (over y, core), rep: 8 (over z, x).
Axes of the slice: x: 2, y: 2, z: 4, core: 2. Of those that a mesh axis runs over, the one named last changes fastest.
Arguments:
- facts: float32 [131072, 256], P(('dom', 'rep')), may hold values from -6 to 6
- row_owner: int32 [131072, 1], P(('dom', 'rep')), may hold values from 0 to 3; in each aligned block of 4096 rows (0 to 4095, 4096 to 8191, ...) at most 2048 rows name the same one
- key_offset: int32 [131072], P(('dom', 'rep')), may hold values from 0 to 1023
Outputs:
- key_means: float32 [4096, 256], P(('dom', 'rep'))
- key_counts: float32 [4096], P(('dom', 'rep'))
The draws below stay inside these ranges and needn't reach their ends.
Inputs may be any that keep to these rules, and one draw needn't show every extreme that they name: `row_owner`: in the rows of one device no key range is named by more than 2048 rows, a bound that some block reaches.
All inputs are finite; a program needn't handle non-finite values.
Results may differ from the reference program's by a relative error of at most 0.0003.
Values sent between devices are 32-bit elements; how exact they have to be, the bound alone decides.
A program may use at most 64 MiB of HBM per device.

```python
import math
import jax
import jax.numpy as jnp
import numpy as np

M = 256
KEYS = 4096
ROWS_DEV = 4096
ROWS = 131072
RANGE = 1024
CAP = 2048
N_DOM = 4


def draw_key_offset(key, part):
    order_key = jax.random.fold_in(key, 11)
    kept_key = jax.random.fold_in(key, 12)
    first_key = jax.random.fold_in(key, 13)
    second_key = jax.random.fold_in(key, 14)
    inner_offsets = (jax.random.permutation(order_key, RANGE - 2) + 1).astype(jnp.int32)
    end_offsets = jnp.array([0, RANGE - 1], jnp.int32)
    kept_offsets = jnp.concatenate([end_offsets, inner_offsets[4:]])
    kept_offsets = jax.random.permutation(kept_key, kept_offsets).astype(jnp.int32)
    first_draw = jax.random.randint(first_key, (ROWS,), 0, RANGE - 4, dtype=jnp.int32)
    second_draw = jax.random.randint(second_key, (ROWS,), 0, RANGE - 4, dtype=jnp.int32)
    return kept_offsets[jnp.minimum(first_draw, second_draw)].astype(jnp.int32)


def block_levels(rng, shape, shards, least, top_value):
    factor_of = 1.0
    for axis_at, parts in shards:
        steps = jax.random.uniform(jax.random.fold_in(jax.random.fold_in(rng, 6), axis_at), (parts,), jnp.float32, least / len(shards), top_value / len(shards))
        factor_of = factor_of * jnp.repeat(jnp.exp(steps), shape[axis_at] // parts).reshape((-1,) + (1,) * (len(shape) - 1 - axis_at))
    return factor_of


def shared_out(stream_key, own, number, rows, amount, top, reach, skew):
    order = jax.random.permutation(stream_key, amount)
    packed, usual = shares(amount, rows * top, reach, skew, True), shares(amount, rows * top, reach, skew, False)
    places = jnp.arange(amount)

    def named(tallies, rotation):
        used = int((tallies > 0).sum())
        fixed = max(1, used // 4)
        shifted = fixed + (places - fixed + rotation * (used - fixed)) % max(1, amount - fixed)
        return jnp.zeros((amount,), jnp.int32).at[order[jnp.where(places < fixed, places, shifted)]].set(jnp.asarray(tallies, jnp.int32))

    tallies = jnp.where(number % 4 == 0, named(packed, number // 4), named(usual, number - number // 4 - 1))
    mixed = jax.random.permutation(jax.random.fold_in(own, 3), amount)
    source_of, taker = mixed[0:amount // 2 * 2:2], mixed[1:amount // 2 * 2:2]
    slack = jnp.minimum(tallies[source_of] - 1, reach - tallies[taker]) // 2
    slack = jnp.where((source_of == order[0]) | (taker == order[0]) | (tallies[taker] == 0), 0, jnp.maximum(slack, 0))
    shifted = jax.random.randint(jax.random.fold_in(own, 4), (amount // 2,), 0, 1 << 20) % (slack + 1)
    tallies = tallies.at[source_of].add(-shifted).at[taker].add(shifted)
    items = jnp.searchsorted(jnp.cumsum(tallies), jnp.arange(rows * top), side="right").astype(jnp.int32)
    grid = items.reshape(top, rows).T
    grid = grid[jax.random.permutation(jax.random.fold_in(own, 1), rows)]
    rotation = jax.random.randint(jax.random.fold_in(own, 2), (rows, 1), 0, top)
    return jnp.take_along_axis(grid, (jnp.arange(top)[None, :] + rotation) % top, axis=1)


def shares(count, total, most, slope, full):
    portions = [(1 << 20) // math.isqrt(grade ** slope) + 1 for grade in range(1, count + 1)]
    largest = most if full else min(most, max(-(-total // count), total * portions[0] // sum(portions)))
    least = 1 if total - largest >= count - 1 else 0
    holding, rest = [largest] + [least] * (count - 1), total - largest - least * (count - 1)
    while rest > 0:
        free = [i for i in range(1, count) if holding[i] < largest] or [i for i in range(1, count) if holding[i] < most]
        mass, remaining = sum([portions[i] for i in free]), rest
        for i in free:
            more = min(most - holding[i], max(1, remaining * portions[i] // mass), rest)
            holding[i] = holding[i] + more
            rest = rest - more
    return np.array(holding)


def centred(own_key, extent, deviation, bound, split=(), held_as=jnp.bfloat16):
    result = deviation * jax.random.normal(own_key, extent, jnp.float32)
    if split:
        result = result * block_levels(own_key, extent, split, -0.22, 0.18)
    return jnp.clip(result, -bound, bound).astype(held_as)


def setup_inputs(seed: int = 0) -> dict:
    splits = jax.random.split(jax.random.key(seed), 4)
    facts = centred(splits[0], (ROWS, M), 1.0, 6.0, ((0, 32),), jnp.float32)
    row_owner_keys = jax.random.split(jax.random.fold_in(splits[1], 1), ROWS // ROWS_DEV)
    row_owner_turns = jax.random.permutation(jax.random.fold_in(splits[1], 3), ROWS // ROWS_DEV)
    row_owner = jax.vmap(lambda own, number: shared_out(jax.random.fold_in(splits[1], 2), own, number, ROWS_DEV, N_DOM, 1, CAP, 2))(row_owner_keys, row_owner_turns).reshape((ROWS, 1))
    key_offset = draw_key_offset(jax.random.fold_in(splits[3], 71), 0)
    return dict(facts=facts, row_owner=row_owner, key_offset=key_offset)


def reference(facts, row_owner, key_offset):
    key_ids = row_owner[:, 0] * (KEYS // N_DOM) + key_offset
    key_sums = jax.ops.segment_sum(facts, key_ids, num_segments=KEYS)
    key_counts = jax.ops.segment_sum(jnp.ones(key_ids.shape, jnp.float32), key_ids, num_segments=KEYS)
    key_means = key_sums / jnp.maximum(key_counts, 1.0)[:, None]
    return key_means, key_counts
```

```python
import functools

import jax
import jax.numpy as jnp
from jax import lax
from jax.experimental import pallas as pl
from jax.experimental.pallas import tpu as pltpu
from jax.sharding import PartitionSpec as P

KEYS = 4096
MESH = pl.DeviceIdType.MESH
F32 = jnp.float32
BF16 = jnp.bfloat16


def flip(index, bits):
    at = 1
    while at <= bits:
        if bits & at:
            index = index + at * (1 - 2 * ((index // at) % 2))
        at *= 2
    return index


def kernel(D, Z, hb, rows, M, chunk, lab_ref, crow_ref, ccol_ref, facts_ref, out_ref, cout_ref,
           fbuf, X, sendC1, sendC2, recvC1, recvC2, acc1, acc2,
           rA1, rB1, rA2, rB2, rZ,
           c0, cS, cR, cD, cX, cXr, cZ, cZr, fsem,
           sC1, tC1, sC2, tC2, sA1, tA1, sB1, tB1, sA2, tA2, sB2, tB2, sZ, tZ,
           scC, tcC, scD, tcD, scX, tcX, scZ, tcZ):
    me_d, me_r = lax.axis_index("dom"), lax.axis_index("rep")
    T1, T2 = (3 * D - 2) * hb, (D + 2) * hb
    stage = 4 * D * hb
    core = (flip(me_d, 1), me_r)
    dpeer = [None] + [(flip(me_d, 2 * d), me_r) for d in range(1, D)]
    xpeer = (me_d, flip(me_r, 1))
    zpeer = [None] + [(me_d, flip(me_r, 2 * z)) for z in range(1, Z)]
    peers = [core] + dpeer[1:] + [xpeer] + zpeer[1:]

    nchunks = rows // chunk
    loads = [
        pltpu.make_async_copy(
            facts_ref.at[pl.ds(k * chunk, chunk)], fbuf.at[pl.ds(k * chunk, chunk)], fsem.at[k]
        )
        for k in range(nchunks)
    ]
    for ld in loads:
        ld.start()
    barrier = pltpu.get_barrier_semaphore()
    for p in peers:
        pl.semaphore_signal(barrier, inc=1, device_id=p, device_id_type=MESH)

    def rcopy(src, dst, s, t, dev):
        return pltpu.make_async_remote_copy(
            src_ref=src, dst_ref=dst, send_sem=s, recv_sem=t, device_id=dev, device_id_type=MESH
        )

    nrow = 4 * D * Z
    kpd = 2 * hb
    hot_r = jnp.where(lax.broadcasted_iota(jnp.int32, (nrow, rows), 0) == crow_ref[...], 1.0, 0.0).astype(BF16)
    hot_c = jnp.where(lax.broadcasted_iota(jnp.int32, (kpd, rows), 0) == ccol_ref[...], 1.0, 0.0).astype(BF16)
    cnt = lax.dot_general(hot_r, hot_c, (((1,), (1,)), ((), ())), preferred_element_type=F32)
    half = nrow // 2
    for d in range(D):
        c0[d] = cnt[d * 2 * Z:(d + 1) * 2 * Z]
        cS[d] = cnt[half + d * 2 * Z:half + (d + 1) * 2 * Z]

    for k in range(nchunks):
        loads[k].wait()

        @pl.loop(0, chunk // 256)
        def _(j):
            at = pl.multiple_of(k * chunk + j * 256, 256)
            v = fbuf[pl.ds(at, 256), :]
            hi = v.astype(BF16)
            X[pl.ds(at, 256), 0:M] = hi
            X[pl.ds(at, 256), M:2 * M] = (v - hi.astype(F32)).astype(BF16)

    pl.semaphore_wait(barrier, len(peers))
    cc = rcopy(cS, cR, scC, tcC, core)
    cc.start()

    def tile(start, size):
        rel = lab_ref[...] - start
        total = None
        for k in range(nchunks):
            part = rel[:, k * chunk:(k + 1) * chunk]
            hot = jnp.where(lax.broadcasted_iota(jnp.int32, (size, chunk), 0) == part, 1.0, 0.0).astype(BF16)
            o = jnp.dot(hot, X[k * chunk:(k + 1) * chunk, :], preferred_element_type=F32)
            total = o if total is None else total + o
        return total[:, 0:M] + total[:, M:2 * M]

    def C1(i):
        return rcopy(sendC1.at[i], recvC1.at[i], sC1.at[i], tC1.at[i], core)

    def C2(i):
        return rcopy(sendC2.at[i], recvC2.at[i], sC2.at[i], tC2.at[i], core)

    def A1(i, d):
        return rcopy(acc1.at[i, pl.ds(2 * (d - 1) * hb, 2 * hb)], rA1.at[i, d - 1],
                     sA1.at[i, d - 1], tA1.at[i, d - 1], dpeer[d])

    def B1(i):
        return rcopy(acc1.at[i, pl.ds(2 * (D - 1) * hb, D * hb)], rB1.at[i], sB1.at[i], tB1.at[i], xpeer)

    def A2(i):
        return rcopy(acc2.at[i, pl.ds(0, hb)], rA2.at[i], sA2.at[i], tA2.at[i], xpeer)

    def B2(i, d):
        return rcopy(acc2.at[i, pl.ds(d * hb, hb)], rB2.at[i, d - 1], sB2.at[i, d - 1], tB2.at[i, d - 1], dpeer[d])

    def ZC(i, z):
        return rcopy(acc2.at[i, pl.ds(D * hb, 2 * hb)], rZ.at[i], sZ.at[i], tZ.at[i], zpeer[z])

    def phase1(i):
        C1(i).wait_recv()
        acc1[i] = acc1[i] + recvC1[i]
        for d in range(1, D):
            A1(i, d).start()
        B1(i).start()

    def core2(i):
        C2(i).wait_recv()
        acc2[i] = acc2[i] + recvC2[i]

    def phase2(i):
        x0 = pl.ds(D * hb, hb)
        for d in range(1, D):
            A1(i, d).wait_recv()
            acc2[i, 0:hb] = acc2[i, 0:hb] + rA1[i, d - 1, hb:2 * hb]
        A2(i).start()
        B1(i).wait_recv()
        for d in range(1, D):
            acc2[i, d * hb:(d + 1) * hb] = acc2[i, d * hb:(d + 1) * hb] + rB1[i, d * hb:(d + 1) * hb]
            B2(i, d).start()
        extra = rA1[i, 0, 0:hb]
        for d in range(2, D):
            extra = extra + rA1[i, d - 1, 0:hb]
        acc2[i, x0] = acc2[i, x0] + extra
        b0 = pl.ds((D + 1) * hb, hb)
        acc2[i, b0] = acc2[i, b0] + rB1[i, 0:hb]

    def phase3(i):
        x0 = pl.ds(D * hb, hb)
        b0 = pl.ds((D + 1) * hb, hb)
        A2(i).wait_recv()
        acc2[i, x0] = acc2[i, x0] + rA2[i]
        for d in range(1, D):
            B2(i, d).wait_recv()
            acc2[i, b0] = acc2[i, b0] + rB2[i, d - 1]
        for z in range(1, Z):
            @pl.when(i == Z - 1 - z)
            def _():
                ZC(i, z).start()

    def DC(d):
        return rcopy(c0.at[d], cD.at[d - 1], scD.at[d - 1], tcD.at[d - 1], dpeer[d])

    def XC():
        return rcopy(cX, cXr, scX, tcX, xpeer)

    def ZCc(z):
        return rcopy(cZ, cZr.at[z - 1], scZ.at[z - 1], tcZ.at[z - 1], zpeer[z])

    def count_step(i):
        @pl.when(i == 0)
        def _():
            cc.wait_recv()
            for d in range(D):
                c0[d] = c0[d] + cR[d]
            for d in range(1, D):
                DC(d).start()

        @pl.when(i == 1)
        def _():
            v = c0[0]
            for d in range(1, D):
                DC(d).wait_recv()
                v = v + cD[d - 1]
            cX[...] = v
            XC().start()

        @pl.when(i == 2)
        def _():
            XC().wait_recv()
            cZ[...] = cX[0:Z] + cXr[Z:2 * Z]
            for z in range(1, Z):
                ZCc(z).start()

    @pl.loop(0, Z + 3)
    def _(i):
        @pl.when(i < Z)
        def _():
            base = i * 2 * stage
            sendC1[i] = tile(base + stage, T1)
            C1(i).start()

        @pl.when((i >= 1) & (i <= Z))
        def _():
            core2(i - 1)

        @pl.when((i >= 2) & (i <= Z + 1))
        def _():
            phase2(i - 2)

        @pl.when(i < Z)
        def _():
            base = i * 2 * stage
            acc1[i] = tile(base, T1)
            count_step(i)
            sendC2[i] = tile(base + stage + T1, T2)
            C2(i).start()
            phase1(i)

        @pl.when(i >= 3)
        def _():
            phase3(i - 3)

        @pl.when(i < Z)
        def _():
            acc2[i] = tile(i * 2 * stage + T1, T2)

    cf = cZ[0:1, :]
    for z in range(1, Z):
        ZCc(z).wait_recv()
        cf = cf + cZr[z - 1, z:z + 1, :]
    cout_ref[...] = cf
    spread = jnp.broadcast_to(jnp.maximum(cf, 1.0), (kpd, kpd))
    eye = lax.broadcasted_iota(jnp.int32, (kpd, kpd), 0) == lax.broadcasted_iota(jnp.int32, (kpd, kpd), 1)
    col = jnp.sum(jnp.where(eye, spread, 0.0), axis=1, keepdims=True)
    tot = acc2[Z - 1, D * hb:(D + 2) * hb]
    for i in range(Z - 1):
        ZC(i, Z - 1 - i).wait_recv()
        tot = tot + rZ[i]
    out_ref[...] = tot / col

    cc.wait_send()
    for d in range(1, D):
        DC(d).wait_send()
    XC().wait_send()
    for z in range(1, Z):
        ZCc(z).wait_send()
        ZC(Z - 1 - z, z).wait_send()

    @pl.loop(0, Z)
    def _(i):
        C1(i).wait_send()
        C2(i).wait_send()
        for d in range(1, D):
            A1(i, d).wait_send()
            B2(i, d).wait_send()
        B1(i).wait_send()
        A2(i).wait_send()


def per_device(facts, row_owner, key_offset):
    n_dom, n_rep = lax.axis_size("dom"), lax.axis_size("rep")
    rows, M = facts.shape
    D, Z = n_dom // 2, n_rep // 2
    kpd = KEYS // (n_dom * n_rep)
    hb = kpd // 2
    T1, T2 = (3 * D - 2) * hb, (D + 2) * hb
    owner = row_owner[:, 0]
    rel = owner ^ lax.axis_index("dom")
    dc, d = rel & 1, rel >> 1
    i = key_offset % kpd
    rr = (key_offset // kpd) ^ lax.axis_index("rep")
    x, z = rr & 1, rr >> 1
    h, ii = i // hb, i % hb
    blk_a = jnp.where(d > 0, 2 * (d - 1) + x, jnp.where(x > 0, 3 * D - 2, 4 * D - 2))
    blk_b = jnp.where(x > 0, 2 * (D - 1) + d, jnp.where(d > 0, 3 * D - 2 + d, 4 * D - 1))
    blk = jnp.where(h > 0, blk_b, blk_a)
    label = (((Z - 1 - z) * 2 + dc) * (4 * D) + blk) * hb + ii
    crow = ((dc * D + d) * 2 + x) * Z + z
    chunk = min(1024, rows)

    def vm(*shape, dtype=F32):
        return pltpu.VMEM(shape, dtype)

    def dma(*shape):
        return [pltpu.SemaphoreType.DMA(shape)] * 2 if shape else [pltpu.SemaphoreType.DMA] * 2

    scratch = [
        vm(rows, M), vm(rows, 2 * M, dtype=BF16),
        vm(Z, T1, M), vm(Z, T2, M), vm(Z, T1, M), vm(Z, T2, M), vm(Z, T1, M), vm(Z, T2, M),
        vm(Z, D - 1, 2 * hb, M), vm(Z, D * hb, M), vm(Z, hb, M), vm(Z, D - 1, hb, M), vm(Z - 1, 2 * hb, M),
        vm(D, 2 * Z, kpd), vm(D, 2 * Z, kpd), vm(D, 2 * Z, kpd), vm(D - 1, 2 * Z, kpd),
        vm(2 * Z, kpd), vm(2 * Z, kpd), vm(Z, kpd), vm(Z - 1, Z, kpd),
        pltpu.SemaphoreType.DMA((rows // chunk,)),
        *dma(Z), *dma(Z), *dma(Z, D - 1), *dma(Z), *dma(Z), *dma(Z, D - 1), *dma(Z - 1),
        *dma(), *dma(D - 1), *dma(), *dma(Z - 1),
    ]
    vmem = pl.BlockSpec(memory_space=pltpu.VMEM)
    means, counts = pl.pallas_call(
        functools.partial(kernel, D, Z, hb, rows, M, chunk),
        out_shape=(jax.ShapeDtypeStruct((kpd, M), F32), jax.ShapeDtypeStruct((1, kpd), F32)),
        in_specs=[vmem, vmem, vmem, pl.BlockSpec(memory_space=pl.ANY)],
        out_specs=(vmem, vmem),
        scratch_shapes=scratch,
        compiler_params=pltpu.CompilerParams(
            collective_id=0, has_side_effects=True, vmem_limit_bytes=50 * 1024 * 1024
        ),
    )(label[None, :], crow[None, :], i[None, :], facts)
    return means, counts.reshape(kpd)


def solution(mesh):
    placed = (P(("dom", "rep"), None), P(("dom", "rep"), None), P(("dom", "rep")))
    return jax.shard_map(
        per_device,
        mesh=mesh,
        in_specs=placed,
        out_specs=(P(("dom", "rep"), None), P(("dom", "rep"))),
        check_vma=False,
    )
```

```python
import functools

import jax
import jax.numpy as jnp
from jax import lax
from jax.experimental import pallas as pl
from jax.experimental.pallas import tpu as pltpu
from jax.sharding import PartitionSpec as P

KEYS = 4096
MESH = pl.DeviceIdType.MESH
F32 = jnp.float32
BF16 = jnp.bfloat16


def flip(index, bits):
    at = 1
    while at <= bits:
        if bits & at:
            index = index + at * (1 - 2 * ((index // at) % 2))
        at *= 2
    return index


def kernel(D, Z, hb, rows, M, chunk, owner_hbm, offset_hbm, facts_ref, out_ref, cout_ref,
           owner_ref, offset_ref, lab_ref, fbuf, high, low, tab, recvC1, recvC2,
           rA1, rB1, rA2, rB2, rZ,
           c0, cS, cR, cD, cX, cXr, cZ, cZr, fsem, isem,
           sC1, tC1, sC2, tC2, sA1, tA1, sB1, tB1, sA2, tA2, sB2, tB2, sZ, tZ,
           scC, tcC, scD, tcD, scX, tcX, scZ, tcZ):
    me_d, me_r = lax.axis_index("dom"), lax.axis_index("rep")
    T1, T2 = (3 * D - 2) * hb, (D + 2) * hb
    stage = 4 * D * hb
    core = (flip(me_d, 1), me_r)
    dpeer = [None] + [(flip(me_d, 2 * d), me_r) for d in range(1, D)]
    xpeer = (me_d, flip(me_r, 1))
    zpeer = [None] + [(me_d, flip(me_r, 2 * z)) for z in range(1, Z)]
    peers = [core] + dpeer[1:] + [xpeer] + zpeer[1:]

    nchunks = rows // chunk
    loads = [
        pltpu.make_async_copy(
            facts_ref.at[pl.ds(k * chunk, chunk)], fbuf.at[pl.ds(k * chunk, chunk)], fsem.at[k]
        )
        for k in range(nchunks)
    ]
    ints = [
        pltpu.make_async_copy(owner_hbm, owner_ref, isem.at[0]),
        pltpu.make_async_copy(offset_hbm, offset_ref, isem.at[1]),
    ]
    for ld in ints + loads:
        ld.start()
    barrier = pltpu.get_barrier_semaphore()
    for p in peers:
        pl.semaphore_signal(barrier, inc=1, device_id=p, device_id_type=MESH)

    def rcopy(src, dst, s, t, dev):
        return pltpu.make_async_remote_copy(
            src_ref=src, dst_ref=dst, send_sem=s, recv_sem=t, device_id=dev, device_id_type=MESH
        )

    nrow = 4 * D * Z
    kpd = 2 * hb
    for ld in ints:
        ld.wait()
    rel = owner_ref[...] ^ me_d
    dc, d = rel & 1, rel >> 1
    offset = offset_ref[...]
    i = offset & (kpd - 1)
    rr = (offset >> (kpd.bit_length() - 1)) ^ me_r
    x, z = rr & 1, rr >> 1
    ii = i & (hb - 1)
    blk_a = jnp.where(d > 0, 2 * (d - 1) + x, jnp.where(x > 0, 3 * D - 2, 4 * D - 2))
    blk_b = jnp.where(x > 0, 2 * (D - 1) + d, jnp.where(d > 0, 3 * D - 2 + d, 4 * D - 1))
    blk = jnp.where(i >= hb, blk_b, blk_a)
    lab_ref[...] = (((Z - 1 - z) * 2 + dc) * (4 * D) + blk) * hb + ii
    crow = ((dc * D + d) * 2 + x) * Z + z
    hot_r = jnp.where(lax.broadcasted_iota(jnp.int32, (nrow, rows), 0) == crow, 1.0, 0.0).astype(BF16)
    hot_c = jnp.where(lax.broadcasted_iota(jnp.int32, (kpd, rows), 0) == i, 1.0, 0.0).astype(BF16)
    cnt = lax.dot_general(hot_r, hot_c, (((1,), (1,)), ((), ())), preferred_element_type=F32)
    half = nrow // 2
    for d in range(D):
        c0[d] = cnt[d * 2 * Z:(d + 1) * 2 * Z]
        cS[d] = cnt[half + d * 2 * Z:half + (d + 1) * 2 * Z]

    for k in range(nchunks):
        loads[k].wait()

        @pl.loop(0, chunk // 256)
        def _(j):
            at = pl.multiple_of(k * chunk + j * 256, 256)
            v = fbuf[pl.ds(at, 256), :]
            hi = v.astype(BF16)
            high[pl.ds(at, 256), :] = hi
            low[pl.ds(at, 256), :] = (v - hi.astype(F32)).astype(BF16)

    pl.semaphore_wait(barrier, len(peers))
    cc = rcopy(cS, cR, scC, tcC, core)
    cc.start()

    def tile(start, size):
        rel = lab_ref[...] - start
        total = None
        for k in range(nchunks):
            part = rel[:, k * chunk:(k + 1) * chunk]
            hot = jnp.where(lax.broadcasted_iota(jnp.int32, (size, chunk), 0) == part, 1.0, 0.0).astype(BF16)
            at = slice(k * chunk, (k + 1) * chunk)
            o = jnp.dot(hot, high[at, :], preferred_element_type=F32) + jnp.dot(
                hot, low[at, :], preferred_element_type=F32
            )
            total = o if total is None else total + o
        return total

    def C1(i):
        return rcopy(tab.at[4 * i, pl.ds(0, T1)], recvC1.at[i], sC1.at[i], tC1.at[i], core)

    def C2(i):
        return rcopy(tab.at[4 * i + 2, pl.ds(0, T2)], recvC2.at[i], sC2.at[i], tC2.at[i], core)

    def A1(i, d):
        return rcopy(tab.at[4 * i + 1, pl.ds(2 * (d - 1) * hb, 2 * hb)], rA1.at[i, d - 1],
                     sA1.at[i, d - 1], tA1.at[i, d - 1], dpeer[d])

    def B1(i):
        return rcopy(tab.at[4 * i + 1, pl.ds(2 * (D - 1) * hb, D * hb)], rB1.at[i], sB1.at[i], tB1.at[i], xpeer)

    def A2(i):
        return rcopy(tab.at[4 * i + 3, pl.ds(0, hb)], rA2.at[i], sA2.at[i], tA2.at[i], xpeer)

    def B2(i, d):
        return rcopy(tab.at[4 * i + 3, pl.ds(d * hb, hb)], rB2.at[i, d - 1], sB2.at[i, d - 1], tB2.at[i, d - 1], dpeer[d])

    def ZC(i, z):
        return rcopy(tab.at[4 * i + 3, pl.ds(D * hb, 2 * hb)], rZ.at[i], sZ.at[i], tZ.at[i], zpeer[z])

    def phase1(i):
        C1(i).wait_recv()
        tab[4 * i + 1, 0:T1] = tab[4 * i + 1, 0:T1] + recvC1[i]
        for d in range(1, D):
            A1(i, d).start()
        B1(i).start()

    def core2(i):
        C2(i).wait_recv()
        tab[4 * i + 3, 0:T2] = tab[4 * i + 3, 0:T2] + recvC2[i]

    def phase2(i):
        x0 = pl.ds(D * hb, hb)
        for d in range(1, D):
            A1(i, d).wait_recv()
            tab[4 * i + 3, 0:hb] = tab[4 * i + 3, 0:hb] + rA1[i, d - 1, hb:2 * hb]
        A2(i).start()
        B1(i).wait_recv()
        for d in range(1, D):
            tab[4 * i + 3, d * hb:(d + 1) * hb] = tab[4 * i + 3, d * hb:(d + 1) * hb] + rB1[i, d * hb:(d + 1) * hb]
            B2(i, d).start()
        extra = rA1[i, 0, 0:hb]
        for d in range(2, D):
            extra = extra + rA1[i, d - 1, 0:hb]
        tab[4 * i + 3, x0] = tab[4 * i + 3, x0] + extra
        b0 = pl.ds((D + 1) * hb, hb)
        tab[4 * i + 3, b0] = tab[4 * i + 3, b0] + rB1[i, 0:hb]

    def phase3(i):
        x0 = pl.ds(D * hb, hb)
        b0 = pl.ds((D + 1) * hb, hb)
        A2(i).wait_recv()
        tab[4 * i + 3, x0] = tab[4 * i + 3, x0] + rA2[i]
        for d in range(1, D):
            B2(i, d).wait_recv()
            tab[4 * i + 3, b0] = tab[4 * i + 3, b0] + rB2[i, d - 1]
        for z in range(1, Z):
            if isinstance(i, int):
                if i == Z - 1 - z:
                    ZC(i, z).start()
                continue

            @pl.when(i == Z - 1 - z)
            def _():
                ZC(i, z).start()

    def DC(d):
        return rcopy(c0.at[d], cD.at[d - 1], scD.at[d - 1], tcD.at[d - 1], dpeer[d])

    def XC():
        return rcopy(cX, cXr, scX, tcX, xpeer)

    def ZCc(z):
        return rcopy(cZ, cZr.at[z - 1], scZ.at[z - 1], tcZ.at[z - 1], zpeer[z])

    def count_step(i):
        @pl.when(i == 0)
        def _():
            cc.wait_recv()
            for d in range(D):
                c0[d] = c0[d] + cR[d]
            for d in range(1, D):
                DC(d).start()

        @pl.when(i == 1)
        def _():
            v = c0[0]
            for d in range(1, D):
                DC(d).wait_recv()
                v = v + cD[d - 1]
            cX[...] = v
            XC().start()

        @pl.when(i == 2)
        def _():
            XC().wait_recv()
            cZ[...] = cX[0:Z] + cXr[Z:2 * Z]
            for z in range(1, Z):
                ZCc(z).start()

    @pl.loop(0, 4 * Z)
    def _(t):
        i, j = t // 4, t % 4
        tab[t] = tile((2 * i + 1 - j % 2) * stage + (j // 2) * T1, max(T1, T2))

        @pl.when(j == 0)
        def _():
            C1(i).start()

        @pl.when((j == 0) & (i >= 1))
        def _():
            core2(i - 1)

        @pl.when(j == 1)
        def _():
            phase1(i)
            count_step(i)

        @pl.when(j == 2)
        def _():
            C2(i).start()

        @pl.when((j == 2) & (i >= 1))
        def _():
            phase2(i - 1)

        @pl.when((j == 3) & (i >= 2))
        def _():
            phase3(i - 2)

    core2(Z - 1)
    phase2(Z - 1)
    phase3(Z - 2)
    phase3(Z - 1)
    cf = cZ[0:1, :]
    for z in range(1, Z):
        ZCc(z).wait_recv()
        cf = cf + cZr[z - 1, z:z + 1, :]
    cout_ref[...] = cf
    spread = jnp.broadcast_to(jnp.maximum(cf, 1.0), (kpd, kpd))
    eye = lax.broadcasted_iota(jnp.int32, (kpd, kpd), 0) == lax.broadcasted_iota(jnp.int32, (kpd, kpd), 1)
    col = jnp.sum(jnp.where(eye, spread, 0.0), axis=1, keepdims=True)
    tot = tab[4 * Z - 1, D * hb:(D + 2) * hb]
    for i in range(Z - 1):
        ZC(i, Z - 1 - i).wait_recv()
        tot = tot + rZ[i]
    out_ref[...] = tot / col

    cc.wait_send()
    for d in range(1, D):
        DC(d).wait_send()
    XC().wait_send()
    for z in range(1, Z):
        ZCc(z).wait_send()
        ZC(Z - 1 - z, z).wait_send()

    @pl.loop(0, Z)
    def _(i):
        C1(i).wait_send()
        C2(i).wait_send()
        for d in range(1, D):
            A1(i, d).wait_send()
            B2(i, d).wait_send()
        B1(i).wait_send()
        A2(i).wait_send()


def per_device(facts, row_owner, key_offset):
    n_dom, n_rep = lax.axis_size("dom"), lax.axis_size("rep")
    rows, M = facts.shape
    D, Z = n_dom // 2, n_rep // 2
    kpd = KEYS // (n_dom * n_rep)
    hb = kpd // 2
    T1, T2 = (3 * D - 2) * hb, (D + 2) * hb
    chunk = min(1024, rows)

    def vm(*shape, dtype=F32):
        return pltpu.VMEM(shape, dtype)

    def dma(*shape):
        return [pltpu.SemaphoreType.DMA(shape)] * 2 if shape else [pltpu.SemaphoreType.DMA] * 2

    scratch = [
        vm(1, rows, dtype=jnp.int32), vm(1, rows, dtype=jnp.int32), vm(1, rows, dtype=jnp.int32),
        vm(rows, M), vm(rows, M, dtype=BF16), vm(rows, M, dtype=BF16),
        vm(4 * Z, max(T1, T2), M), vm(Z, T1, M), vm(Z, T2, M),
        vm(Z, D - 1, 2 * hb, M), vm(Z, D * hb, M), vm(Z, hb, M), vm(Z, D - 1, hb, M), vm(Z - 1, 2 * hb, M),
        vm(D, 2 * Z, kpd), vm(D, 2 * Z, kpd), vm(D, 2 * Z, kpd), vm(D - 1, 2 * Z, kpd),
        vm(2 * Z, kpd), vm(2 * Z, kpd), vm(Z, kpd), vm(Z - 1, Z, kpd),
        pltpu.SemaphoreType.DMA((rows // chunk,)), pltpu.SemaphoreType.DMA((2,)),
        *dma(Z), *dma(Z), *dma(Z, D - 1), *dma(Z), *dma(Z), *dma(Z, D - 1), *dma(Z - 1),
        *dma(), *dma(D - 1), *dma(), *dma(Z - 1),
    ]
    vmem = pl.BlockSpec(memory_space=pltpu.VMEM)
    means, counts = pl.pallas_call(
        functools.partial(kernel, D, Z, hb, rows, M, chunk),
        out_shape=(jax.ShapeDtypeStruct((kpd, M), F32), jax.ShapeDtypeStruct((1, kpd), F32)),
        in_specs=[pl.BlockSpec(memory_space=pl.ANY)] * 3,
        out_specs=(vmem, vmem),
        scratch_shapes=scratch,
        compiler_params=pltpu.CompilerParams(
            collective_id=0, has_side_effects=True, vmem_limit_bytes=50 * 1024 * 1024
        ),
    )(row_owner.reshape(1, rows), key_offset.reshape(1, rows), facts)
    return means, counts.reshape(kpd)


def solution(mesh):
    placed = (P(("dom", "rep"), None), P(("dom", "rep"), None), P(("dom", "rep")))
    return jax.shard_map(
        per_device,
        mesh=mesh,
        in_specs=placed,
        out_specs=(P(("dom", "rep"), None), P(("dom", "rep"))),
        check_vma=False,
    )
```
